256 devices in a mesh: rep: 32 (over x, z_lo, y), shard: 8 (over z_hi, core).
Axes of the slice: x: 4, y: 4, z: 8 (z_hi: 4, z_lo: 2; z = z_hi * 2 + z_lo), core: 2. Of those that a mesh axis runs over, the one named last changes fastest.
Arguments:
- params: float32 [32, 1600, 3200], P('rep', None, 'shard'), may hold values from -6 to 6
- momentum: float32 [32, 1600, 3200], P('rep', None, 'shard'), may hold values from -6 to 6
- tokens: bfloat16 [32, 2, 1024, 1600], P('rep', None, 'shard'), may hold values from -6 to 6
- targets: bfloat16 [32, 2, 1024, 3200], P('rep', None, None, 'shard'), may hold values from -6 to 6
- blend_weight: float32 [3200], P('shard'), may hold values from 0.2 to 0.9
Outputs:
- averaged: float32 [1600, 3200], P(None, 'shard')
- blended: float32 [32, 1600, 3200], P('rep', None, 'shard')
The draws below stay inside these ranges and needn't reach their ends.
All inputs are finite; a program needn't handle non-finite values.
Results may differ from the reference program's by a relative error of at most 0.0045.
Values may be sent and summed in bfloat16 or wider, within the bound.
A program may use at most 128 MiB of HBM per device.

```python
import math
import jax
import jax.numpy as jnp
from jax import lax

D = 1600
FFW = 3200
H = 2
TOKS = 1024
REPS = 32


def levels(stream_key, extent, cuts, low, largest):
    def one(position, blocks):
        steps = jax.random.uniform(jax.random.fold_in(jax.random.fold_in(stream_key, 6), position), (blocks,), jnp.float32, low / len(cuts), largest / len(cuts))
        return jnp.repeat(jnp.exp(steps), extent[position] // blocks).reshape((-1,) + (1,) * (len(extent) - position - 1))

    gain = one(*cuts[0])
    for cut in cuts[1:]:
        gain = gain * one(*cut)
    return gain


def scatter_about(stream_key, shape, width, reach, shards=(), dtype=jnp.bfloat16):
    values = width * jax.random.normal(stream_key, shape, jnp.float32)
    if shards:
        values = values * levels(stream_key, shape, shards, -0.22, 0.18)
    return jnp.clip(values, -reach, reach).astype(dtype)


def setup_inputs(seed: int = 0) -> dict:
    arg_keys = jax.random.split(jax.random.key(seed), 6)
    params = scatter_about(arg_keys[0], (REPS, D, FFW), 1.0, 6.0, ((0, 32), (2, 8)), jnp.float32)
    momentum = scatter_about(arg_keys[1], (REPS, D, FFW), 1.0, 6.0, ((0, 32), (2, 8)), jnp.float32)
    tokens = scatter_about(arg_keys[2], (REPS, H, TOKS, D), 1.0, 6.0, ((0, 32), (2, 8)))
    targets = scatter_about(arg_keys[3], (REPS, H, TOKS, FFW), 1.0, 6.0, ((0, 32), (3, 8)))
    blend_weight = jnp.clip(jnp.exp(math.log(0.9) - 1.50407736 * jax.random.uniform(arg_keys[4], (FFW,), jnp.float32) ** levels(arg_keys[4], (FFW,), ((0, 8),), -0.2, 0.2)), 0.2, 0.9)
    return {"params": params, "momentum": momentum, "tokens": tokens, "targets": targets, "blend_weight": blend_weight}


learn_rate = 0.05
momentum_decay = 0.9

def gelu_tanh(value):
    return jax.nn.gelu(value, approximate=True)

def replica(weight, moment, inputs, wanted):
    scaling = 1.0 / jnp.sqrt(jnp.float32(D))
    for local_step in range(H):
        weight_half = weight.astype(jnp.bfloat16)
        pre = jnp.dot(inputs[local_step], weight_half, preferred_element_type=jnp.float32) * scaling
        activation, pullback = jax.vjp(gelu_tanh, pre)
        slope, = pullback(activation - wanted[local_step].astype(jnp.float32))
        hidden_grad = (slope * scaling).astype(jnp.bfloat16)
        gradient = lax.dot_general(inputs[local_step], hidden_grad, (((0,), (0,)), ((), ())), preferred_element_type=jnp.float32)
        moment = momentum_decay * moment + gradient
        weight = weight - learn_rate * moment
    return (weight, moment)

def reference(params, momentum, tokens, targets, blend_weight):
    weights, moments = lax.map(lambda packed: replica(*packed), (params, momentum, tokens, targets))
    averaged = lax.optimization_barrier(jnp.sum(weights, axis=0)) / jnp.float32(REPS)
    mean_moment = lax.optimization_barrier(jnp.sum(moments, axis=0)) / jnp.float32(REPS)
    blended = blend_weight * mean_moment[None] + (1.0 - blend_weight) * moments
    return (averaged, blended)
```

```python
import functools
import math

import jax
import jax.numpy as jnp
from jax import lax
from jax.experimental import pallas as pl
from jax.experimental.pallas import tpu as pltpu
from jax.sharding import PartitionSpec as P

D = 1600
COLS = 400
REPS = 32
LANES = 128
UNIT = 160
GROUPS = 3
TAIL = 16
TAILROWS = 200
PIECE = 64

learn_rate = 0.05
momentum_decay = 0.9

MESH = pl.DeviceIdType.MESH
F32 = jnp.float32
BF16 = jnp.bfloat16


def rem(value, count):
    return lax.rem(value, jnp.int32(count))


class Sum:
    sizes = dict(own=32, far=8, mid=8, near=16, part=8, cross=6, pair=2, other=2, full=32)

    def __init__(self, refs, rows, place, sends):
        names = list(self.sizes)
        for name, ref in zip(names, refs[: len(names)]):
            setattr(self, name, ref)
        self.send, self.recv = refs[len(names) :]
        self.rows = rows
        self.sends = sends
        self.count = 0
        self.rings, self.pair_id = place

    @classmethod
    def scratch(cls, rows):
        return [pltpu.VMEM((n, rows, LANES), BF16) for n in cls.sizes.values()] + [
            pltpu.SemaphoreType.DMA((38,)),
            pltpu.SemaphoreType.DMA((38,)),
        ]

    def go(self, slot, src, dst, device):
        copy = pltpu.make_async_remote_copy(
            src_ref=src,
            dst_ref=dst,
            send_sem=self.send.at[slot],
            recv_sem=self.recv.at[slot],
            device_id=device,
            device_id_type=MESH,
        )
        copy.start()
        self.sends.append(copy)

    def got(self, slot, dst):
        pltpu.make_async_remote_copy(
            src_ref=dst,
            dst_ref=dst,
            send_sem=self.send.at[slot],
            recv_sem=self.recv.at[slot],
            device_id=self.pair_id,
            device_id_type=MESH,
        ).wait_recv()

    def halves(self):
        for h in range(2):
            (i1, peer1), (i2, peer2) = self.rings if h == 0 else self.rings[::-1]
            yield h, i1, peer1, i2, peer2

    def s1(self):
        for h, i1, peer1, i2, peer2 in self.halves():
            base = 16 * h + 4 * rem(i1 + 2, 4)
            self.go(2 * h, self.own.at[pl.ds(base, 2)], self.far.at[pl.ds(4 * h, 2)], peer1(1))
            self.go(2 * h + 1, self.own.at[pl.ds(base + 2, 2)], self.far.at[pl.ds(4 * h + 2, 2)], peer1(3))
        for h, i1, peer1, i2, peer2 in self.halves():
            right = 16 * h + 4 * rem(i1 + 1, 4)
            left = 16 * h + 4 * rem(i1 + 3, 4)
            self.go(4 + 2 * h, self.own.at[pl.ds(right + 2, 2)], self.near.at[pl.ds(8 * h + 2, 2)], peer1(1))
            self.go(5 + 2 * h, self.own.at[pl.ds(left, 2)], self.near.at[pl.ds(8 * h + 4, 2)], peer1(3))

    def s2(self):
        for h, i1, peer1, i2, peer2 in self.halves():
            right = 16 * h + 4 * rem(i1 + 1, 4)
            left = 16 * h + 4 * rem(i1 + 3, 4)
            for side, first, at in ((0, right, 0), (1, left + 2, 6)):
                mid = self.mid.at[pl.ds(4 * h + 2 * side, 2)]
                self.got(2 * h + side, self.far.at[pl.ds(4 * h + 2 * side, 2)])
                mid[...] = (
                    self.own[pl.ds(first, 2)].astype(F32) + self.far[pl.ds(4 * h + 2 * side, 2)].astype(F32)
                ).astype(BF16)
                self.go(8 + 2 * h + side, mid, self.near.at[pl.ds(8 * h + at, 2)], peer1(1 + 2 * side))

    def s3(self):
        for h, i1, peer1, i2, peer2 in self.halves():
            self.got(4 + 2 * h, self.near.at[pl.ds(8 * h + 2, 2)])
            self.got(5 + 2 * h, self.near.at[pl.ds(8 * h + 4, 2)])
            self.got(8 + 2 * h, self.near.at[pl.ds(8 * h, 2)])
            self.got(9 + 2 * h, self.near.at[pl.ds(8 * h + 6, 2)])
            mine = 16 * h + 4 * i1
            self.part[pl.ds(4 * h, 4)] = (
                self.own[pl.ds(mine, 4)].astype(F32)
                + self.near[pl.ds(8 * h, 4)].astype(F32)
                + self.near[pl.ds(8 * h + 4, 4)].astype(F32)
            ).astype(BF16)
            for d in range(1, 4):
                self.go(
                    12 + 3 * h + d - 1,
                    self.part.at[pl.ds(4 * h + rem(i2 + d, 4), 1)],
                    self.cross.at[pl.ds(3 * h + d - 1, 1)],
                    peer2(d),
                )

    def s4(self):
        for h, i1, peer1, i2, peer2 in self.halves():
            total = self.part[4 * h + i2].astype(F32)
            for d in range(1, 4):
                self.got(12 + 3 * h + d - 1, self.cross.at[pl.ds(3 * h + d - 1, 1)])
                total = total + self.cross[3 * h + d - 1].astype(F32)
            self.pair[h] = total.astype(BF16)
            self.go(18 + h, self.pair.at[pl.ds(h, 1)], self.other.at[pl.ds(h, 1)], self.pair_id)

    def s5(self):
        for h, i1, peer1, i2, peer2 in self.halves():
            self.got(18 + h, self.other.at[pl.ds(h, 1)])
            mine = 16 * h + 4 * i1 + i2
            self.full[mine] = (self.pair[h].astype(F32) + self.other[h].astype(F32)).astype(BF16)
            for d in range(1, 4):
                self.go(20 + 3 * h + d - 1, self.full.at[pl.ds(mine, 1)], self.full.at[pl.ds(mine, 1)], peer2(d))

    def s6(self):
        for h, i1, peer1, i2, peer2 in self.halves():
            mine = 16 * h + 4 * i1
            for d in range(1, 4):
                self.got(20 + 3 * h + d - 1, self.full.at[pl.ds(mine + rem(i2 + 4 - d, 4), 1)])
            low, high = self.full.at[pl.ds(mine, 2)], self.full.at[pl.ds(mine + 2, 2)]
            self.go(26 + 6 * h, low, low, peer1(1))
            self.go(27 + 6 * h, high, high, peer1(3))
            self.go(28 + 6 * h, high, high, peer1(1))
            self.go(29 + 6 * h, low, low, peer1(3))

    def s7(self):
        for h, i1, peer1, i2, peer2 in self.halves():
            low = self.full.at[pl.ds(16 * h + 4 * rem(i1 + 3, 4), 2)]
            high = self.full.at[pl.ds(16 * h + 4 * rem(i1 + 1, 4) + 2, 2)]
            self.got(26 + 6 * h, low)
            self.go(30 + 6 * h, low, low, peer1(1))
            self.got(27 + 6 * h, high)
            self.go(31 + 6 * h, high, high, peer1(3))

    def s8(self):
        for h, i1, peer1, i2, peer2 in self.halves():
            self.got(28 + 6 * h, self.full.at[pl.ds(16 * h + 4 * rem(i1 + 3, 4) + 2, 2)])
            self.got(29 + 6 * h, self.full.at[pl.ds(16 * h + 4 * rem(i1 + 1, 4), 2)])
        for h, i1, peer1, i2, peer2 in self.halves():
            far = 16 * h + 4 * rem(i1 + 2, 4)
            self.got(30 + 6 * h, self.full.at[pl.ds(far, 2)])
            self.got(31 + 6 * h, self.full.at[pl.ds(far + 2, 2)])


def pack(source, own, at, narrow):
    def body(i, carry):
        rows = pl.ds(pl.multiple_of(i * UNIT, UNIT), UNIT)
        for g in range(GROUPS):
            own[10 * g + i, at : at + UNIT, :] = source[rows, LANES * g : LANES * (g + 1)].astype(BF16)
        return carry

    lax.fori_loop(0, 10, body, 0)
    narrow[:, :TAIL] = source[:, LANES * GROUPS :]
    lane = lax.broadcasted_iota(jnp.int32, (TAILROWS, LANES), 1) // TAIL
    packed = jnp.zeros((TAILROWS, LANES), F32)
    for b in range(8):
        part = narrow[TAILROWS * b : TAILROWS * (b + 1), :]
        packed = jnp.where(lane == b, pltpu.roll(part, TAIL * b, 1) if b else part, packed)
    own[30, at : at + UNIT, :] = packed[:UNIT].astype(BF16)
    own[31, at : at + UNIT, :] = jnp.concatenate(
        [packed[UNIT:], jnp.zeros((2 * UNIT - TAILROWS, LANES), F32)], axis=0
    ).astype(BF16)


def kernel(
    w_hbm, m_hbm, tok_hbm, tgt_hbm, bw_ref, avg_hbm, bl_hbm,
    tok, tgt, w, m, g, half, narrow, avg, bl, hg, tsend, trecv, lsem, *sum_refs,
):
    rep, shard = lax.axis_index("rep"), lax.axis_index("shard")
    x, zl, y = rep // 8, rem(rep // 4, 2), rem(rep, 4)
    zh, core = shard // 2, rem(shard, 2)
    right = (rep, 2 * rem(zh + 1, 4) + core)
    left = (rep, 2 * rem(zh + 3, 4) + core)
    partner = (rep, 2 * zh + 1 - core)
    pair_id = (8 * x + 4 * (1 - zl) + y, shard)

    def along_x(d):
        return (8 * rem(x + d, 4) + 4 * zl + y, shard)

    def along_y(d):
        return (8 * x + 4 * zl + rem(y + d, 4), shard)

    sends = []
    place = (((x, along_x), (y, along_y)), pair_id)
    per = len(Sum.sizes) + 2
    first = Sum(sum_refs[:per], 2 * UNIT, place, sends)
    second = Sum(sum_refs[per : 2 * per], UNIT, place, sends)
    third = Sum(sum_refs[2 * per :], UNIT, place, sends)

    loads = [
        pltpu.make_async_copy(tok_hbm.at[0], tok.at[0, 0, pl.ds(2 * core, 2)], lsem.at[0]),
        pltpu.make_async_copy(w_hbm, w, lsem.at[1]),
        pltpu.make_async_copy(m_hbm, m, lsem.at[2]),
        pltpu.make_async_copy(tgt_hbm, tgt, lsem.at[3]),
        pltpu.make_async_copy(tok_hbm.at[1], tok.at[1, 0, pl.ds(2 * core, 2)], lsem.at[4]),
    ]
    for load in loads:
        load.start()
    narrow[...] = jnp.zeros_like(narrow)

    peers = [right, left, partner, pair_id] + [f(d) for f in (along_x, along_y) for d in (1, 2, 3)]
    barrier = pltpu.get_barrier_semaphore()
    for peer in peers:
        pl.semaphore_signal(barrier, inc=1, device_id=peer, device_id_type=MESH)
    pl.semaphore_wait(barrier, len(peers))

    def move(step, slot, src, dst, batch, j, device):
        copy = pltpu.make_async_remote_copy(
            src_ref=src,
            dst_ref=dst,
            send_sem=tsend.at[step, slot],
            recv_sem=trecv.at[step, batch, j],
            device_id=device,
            device_id_type=MESH,
        )
        copy.start()
        sends.append(copy)

    def came(step, batch, j, dst):
        pltpu.make_async_remote_copy(
            src_ref=dst,
            dst_ref=dst,
            send_sem=tsend.at[step, 0],
            recv_sem=trecv.at[step, batch, j],
            device_id=partner,
            device_id_type=MESH,
        ).wait_recv()

    def send_own(step):
        lower, upper = tok.at[step, 0, 2 * core], tok.at[step, 0, 2 * core + 1]
        move(step, 0, lower, tok.at[step, 1, core], 1, core, right)
        move(step, 1, upper, tok.at[step, 1, 2 + core], 1, 2 + core, left)
        move(step, 2, upper, tok.at[step, 2, core], 2, core, right)
        move(step, 3, lower, tok.at[step, 2, 2 + core], 2, 2 + core, left)
        both = tok.at[step, 0, pl.ds(2 * core, 2)]
        move(step, 4, both, both, 0, 2 * core, partner)

    def receive(step, batch):
        if batch == 0:
            came(step, 0, 2 * (1 - core), tok.at[step, 0, pl.ds(2 * (1 - core), 2)])
            return
        for side, onward in ((0, right), (1, left)):
            j = 2 * side + core
            here = tok.at[step, batch, j]
            came(step, batch, j, here)
            if batch == 1:
                move(step, 5 + side, here, tok.at[step, 3, j], 3, j, onward)
            move(step, 5 + 2 * batch + side, here, here, batch, j, partner)

    def receive_partner(step, batch):
        if batch:
            for side in range(2):
                j = 2 * side + 1 - core
                came(step, batch, j, tok.at[step, batch, j])

    scaling = 1.0 / math.sqrt(D)
    root = math.sqrt(2.0 / math.pi)

    def compute(step, batch):
        block = tok[step, batch].reshape(4 * PIECE, D)
        pre = jnp.dot(block, half[...], preferred_element_type=F32) * scaling
        if batch == 0:
            starts = [zh * 256 + 64 * j for j in range(4)]
        else:
            near = {1: (3, 1), 2: (3, 1), 3: (2, 2)}[batch]
            add = {1: (0, 64), 2: (64, 0), 3: (0, 64)}[batch]
            starts = [
                rem(zh + near[side], 4) * 256 + 128 * c + add[side] for side in range(2) for c in range(2)
            ]
        for j, start in enumerate(starts):
            value = pre[PIECE * j : PIECE * (j + 1)]
            wanted = tgt[step, pl.ds(pl.multiple_of(start, PIECE), PIECE), :].astype(F32)
            square = value * value
            curve = jnp.tanh(root * value * (1.0 + 0.044715 * square))
            gate = 0.5 * (1.0 + curve)
            slope = gate + 0.5 * value * (1.0 - curve * curve) * (root * (1.0 + 3 * 0.044715 * square))
            hg[PIECE * j : PIECE * (j + 1), :] = ((value * gate - wanted) * slope * scaling).astype(BF16)
        part = lax.dot_general(block, hg[...], (((0,), (0,)), ((), ())), preferred_element_type=F32)
        if batch == 0:
            g[...] = part
        else:
            g[...] += part

    loads[0].wait()
    send_own(0)
    loads[1].wait()
    half[...] = w[...].astype(BF16)
    pack(w, first.own, 0, narrow)
    loads[2].wait()
    pack(m, first.own, UNIT, narrow)
    first.s1()
    loads[3].wait()
    loads[4].wait()

    receive(0, 0)
    compute(0, 0)
    first.s2()

    receive(0, 1)
    send_own(1)
    receive_partner(0, 1)
    compute(0, 1)
    first.s3()
    first.s4()

    receive(0, 2)
    receive_partner(0, 2)
    compute(0, 2)
    first.s5()
    first.s6()

    receive(0, 3)
    receive_partner(0, 3)
    compute(0, 3)
    m[...] = momentum_decay * m[...] + g[...]
    half[...] = (w[...] - learn_rate * m[...]).astype(BF16)
    pack(g, second.own, 0, narrow)
    second.s1()

    receive(1, 0)
    compute(1, 0)
    first.s7()
    second.s2()

    receive(1, 1)
    receive_partner(1, 1)
    compute(1, 1)
    first.s8()
    second.s3()
    second.s4()

    receive(1, 2)
    receive_partner(1, 2)
    compute(1, 2)
    second.s5()
    second.s6()

    receive(1, 3)
    receive_partner(1, 3)
    compute(1, 3)
    pack(g, third.own, 0, narrow)
    third.s1()

    second.s7()
    m[...] = momentum_decay * m[...] + g[...]
    share = 1.0 / REPS
    second.s8()
    third.s2()

    def sums(unit, rows):
        w0 = first.full[unit, :UNIT][rows].astype(F32)
        m0 = first.full[unit, UNIT:][rows].astype(F32)
        g1 = second.full[unit][rows].astype(F32)
        d = momentum_decay
        average = w0 - learn_rate * ((d + d * d) * m0 + (1.0 + d) * g1)
        return average * share, (d * d * m0 + d * g1) * share

    every = slice(None)

    def base(i, carry):
        rows = pl.ds(pl.multiple_of(i * UNIT, UNIT), UNIT)
        for k in range(GROUPS):
            columns = slice(LANES * k, LANES * (k + 1))
            average, mean = sums(10 * k + i, every)
            part = bw_ref[:, columns]
            avg[rows, columns] = average
            bl[rows, columns] = part * mean + (1.0 - part) * m[rows, columns]
        return carry

    lax.fori_loop(0, 10, base, 0)
    last = slice(LANES * GROUPS, COLS)
    ends = [sums(30, every), sums(31, slice(0, TAILROWS - UNIT))]
    average, mean = (jnp.concatenate([a, b], axis=0) for a, b in zip(*ends))
    part = bw_ref[:, last]
    for b in range(8):
        rows = slice(TAILROWS * b, TAILROWS * (b + 1))
        shift = LANES - TAIL * b
        avg[rows, last] = (pltpu.roll(average, shift, 1) if b else average)[:, :TAIL]
        bl[rows, last] = part * (pltpu.roll(mean, shift, 1) if b else mean)[:, :TAIL] + (1.0 - part) * m[rows, last]

    third.s3()
    third.s4()
    third.s5()
    third.s6()
    third.s7()
    third.s8()

    def finish(i, carry):
        rows = pl.ds(pl.multiple_of(i * UNIT, UNIT), UNIT)
        for k in range(GROUPS):
            columns = slice(LANES * k, LANES * (k + 1))
            total = third.full[10 * k + i].astype(F32) * share
            avg[rows, columns] = avg[rows, columns] - learn_rate * total
            bl[rows, columns] = bl[rows, columns] + bw_ref[:, columns] * total
        return carry

    lax.fori_loop(0, 10, finish, 0)
    total = jnp.concatenate(
        [third.full[30].astype(F32), third.full[31, : TAILROWS - UNIT].astype(F32)], axis=0
    ) * share
    for b in range(8):
        rows = slice(TAILROWS * b, TAILROWS * (b + 1))
        piece = (pltpu.roll(total, LANES - TAIL * b, 1) if b else total)[:, :TAIL]
        avg[rows, last] = avg[rows, last] - learn_rate * piece
        bl[rows, last] = bl[rows, last] + part * piece
    outs = [
        pltpu.make_async_copy(avg, avg_hbm, lsem.at[0]),
        pltpu.make_async_copy(bl, bl_hbm, lsem.at[1]),
    ]
    for out in outs:
        out.start()
    for copy in sends:
        copy.wait_send()
    for out in outs:
        out.wait()


def local(params, momentum, tokens, targets, blend_weight):
    anywhere = pl.BlockSpec(memory_space=pl.ANY)
    averaged, blended = pl.pallas_call(
        kernel,
        out_shape=[jax.ShapeDtypeStruct((D, COLS), F32)] * 2,
        in_specs=[anywhere] * 4 + [pl.BlockSpec(memory_space=pltpu.VMEM)],
        out_specs=[anywhere] * 2,
        scratch_shapes=[
            pltpu.VMEM((2, 4, 4, PIECE, D), BF16),
            pltpu.VMEM((2, 1024, COLS), BF16),
            pltpu.VMEM((D, COLS), F32),
            pltpu.VMEM((D, COLS), F32),
            pltpu.VMEM((D, COLS), F32),
            pltpu.VMEM((D, COLS), BF16),
            pltpu.VMEM((D, LANES), F32),
            pltpu.VMEM((D, COLS), F32),
            pltpu.VMEM((D, COLS), F32),
            pltpu.VMEM((4 * PIECE, COLS), BF16),
            pltpu.SemaphoreType.DMA((2, 13)),
            pltpu.SemaphoreType.DMA((2, 4, 4)),
            pltpu.SemaphoreType.DMA((5,)),
            *Sum.scratch(2 * UNIT),
            *Sum.scratch(UNIT),
            *Sum.scratch(UNIT),
        ],
        compiler_params=pltpu.CompilerParams(
            collective_id=0, has_side_effects=True, vmem_limit_bytes=67043328
        ),
        name="window",
    )(
        params[0],
        momentum[0],
        tokens.reshape(2, 2, PIECE, D),
        targets[0],
        blend_weight.reshape(1, COLS),
    )
    return averaged, blended[None]


def solution(mesh):
    return jax.shard_map(
        local,
        mesh=mesh,
        in_specs=(
            P("rep", None, "shard"),
            P("rep", None, "shard"),
            P("rep", None, "shard", None),
            P("rep", None, None, "shard"),
            P("shard"),
        ),
        out_specs=(P(None, "shard"), P("rep", None, "shard")),
        check_vma=False,
    )
```

```python
import functools
import math

import jax
import jax.numpy as jnp
from jax import lax
from jax.experimental import pallas as pl
from jax.experimental.pallas import tpu as pltpu
from jax.sharding import PartitionSpec as P

D = 1600
COLS = 400
REPS = 32
LANES = 128
SUB = 80
GROUPS = 12
TAIL = 64
TAILROWS = 200
TOKS = 128

learn_rate = 0.05
momentum_decay = 0.9

MESH = pl.DeviceIdType.MESH
F32 = jnp.float32
BF16 = jnp.bfloat16
LAST = slice(GROUPS * LANES, D)


def rem(value, count):
    return lax.rem(value, jnp.int32(count))


class Sum:
    sizes = dict(own=32, far=8, mid=8, near=16, part=8, cross=6, pair=2, other=2, full=32)

    def __init__(self, refs, place, per, wide):
        self.flight = []
        self.per = per
        names = list(self.sizes)
        for name, ref in zip(names, refs[: len(names)]):
            setattr(self, name, ref)
        self.send, self.recv = refs[len(names) :]
        self.wide = wide
        self.rings, self.pair_id = place

    @classmethod
    def scratch(cls, per, wide):
        inner = ("part", "cross")
        return [
            pltpu.VMEM((per * n, SUB, LANES), wide if name in inner else BF16) for name, n in cls.sizes.items()
        ] + [pltpu.SemaphoreType.DMA((9,)), pltpu.SemaphoreType.DMA((7,))]

    def units(self, first, count):
        return pl.ds(self.per * first, self.per * count)

    def copy(self, stage, kind, src, dst, device):
        return pltpu.make_async_remote_copy(
            src_ref=src,
            dst_ref=dst,
            send_sem=self.send.at[stage],
            recv_sem=self.recv.at[kind],
            device_id=device,
            device_id_type=MESH,
        )

    def go(self, stage, kind, src, dst, device):
        self.copy(stage, kind, src, dst, device).start()
        if stage not in self.flight:
            self.flight.append(stage)

    def flush(self):
        for stage in self.flight:
            source, count = ((self.own, 8), (self.own, 8), (self.mid, 8), (self.part, 6), (self.pair, 2), (self.full, 6), (self.full, 8), (self.full, 8), (self.full, 8))[stage]
            all_sent = source.at[self.units(0, count)]
            self.copy(stage, 0, all_sent, all_sent, self.pair_id).wait_send()
        self.flight = []

    def got(self, kind, ref, count):
        everything = ref.at[self.units(0, count)]
        self.copy(0, kind, everything, everything, self.pair_id).wait_recv()

    def halves(self):
        for h in range(2):
            (i1, peer1), (i2, peer2) = self.rings if h == 0 else self.rings[::-1]
            yield h, i1, peer1, i2, peer2

    def s1(self):
        u = self.units
        for h, i1, peer1, i2, peer2 in self.halves():
            base = 16 * h + 4 * rem(i1 + 2, 4)
            self.go(0, 0, self.own.at[u(base, 2)], self.far.at[u(4 * h, 2)], peer1(1))
            self.go(0, 0, self.own.at[u(base + 2, 2)], self.far.at[u(4 * h + 2, 2)], peer1(3))

    def s1b(self):
        u = self.units
        for h, i1, peer1, i2, peer2 in self.halves():
            right = 16 * h + 4 * rem(i1 + 1, 4)
            left = 16 * h + 4 * rem(i1 + 3, 4)
            self.go(1, 1, self.own.at[u(right + 2, 2)], self.near.at[u(8 * h + 2, 2)], peer1(1))
            self.go(1, 1, self.own.at[u(left, 2)], self.near.at[u(8 * h + 4, 2)], peer1(3))

    def s2(self):
        u = self.units
        self.got(0, self.far, 8)
        for h, i1, peer1, i2, peer2 in self.halves():
            right = 16 * h + 4 * rem(i1 + 1, 4)
            left = 16 * h + 4 * rem(i1 + 3, 4)
            for side, first, at in ((0, right, 0), (1, left + 2, 6)):
                here = u(4 * h + 2 * side, 2)
                self.mid[here] = (self.own[u(first, 2)].astype(F32) + self.far[here].astype(F32)).astype(BF16)
                self.go(2, 1, self.mid.at[here], self.near.at[u(8 * h + at, 2)], peer1(1 + 2 * side))

    def s3(self):
        u = self.units
        self.got(1, self.near, 16)
        for h, i1, peer1, i2, peer2 in self.halves():
            mine = 16 * h + 4 * i1
            self.part[u(4 * h, 4)] = (
                self.own[u(mine, 4)].astype(F32)
                + self.near[u(8 * h, 4)].astype(F32)
                + self.near[u(8 * h + 4, 4)].astype(F32)
            ).astype(self.wide)
            for d in range(1, 4):
                self.go(
                    3, 2, self.part.at[u(4 * h + rem(i2 + d, 4), 1)], self.cross.at[u(3 * h + d - 1, 1)], peer2(d)
                )

    def s4(self):
        u = self.units
        self.got(2, self.cross, 6)
        for h, i1, peer1, i2, peer2 in self.halves():
            total = self.part[u(4 * h + i2, 1)].astype(F32)
            for d in range(1, 4):
                total = total + self.cross[u(3 * h + d - 1, 1)].astype(F32)
            self.pair[u(h, 1)] = total.astype(BF16)
            self.go(4, 3, self.pair.at[u(h, 1)], self.other.at[u(h, 1)], self.pair_id)

    def s5(self):
        u = self.units
        self.got(3, self.other, 2)
        for h, i1, peer1, i2, peer2 in self.halves():
            mine = u(16 * h + 4 * i1 + i2, 1)
            self.full[mine] = (self.pair[u(h, 1)].astype(F32) + self.other[u(h, 1)].astype(F32)).astype(BF16)
            for d in range(1, 4):
                self.go(5, 4, self.full.at[mine], self.full.at[mine], peer2(d))

    def sides(self):
        for h, i1, peer1, i2, peer2 in self.halves():
            low, high = (self.full.at[self.units(16 * h + 4 * i1 + at, 2)] for at in (0, 2))
            yield low, high, peer1

    def s6(self):
        self.got(4, self.full, 6)
        for low, high, peer1 in self.sides():
            self.go(6, 5, low, low, peer1(1))
            self.go(6, 5, high, high, peer1(3))

    def s6b(self):
        for low, high, peer1 in self.sides():
            self.go(7, 6, high, high, peer1(1))
            self.go(7, 6, low, low, peer1(3))

    def s7(self):
        u = self.units
        self.got(5, self.full, 8)
        for h, i1, peer1, i2, peer2 in self.halves():
            low = self.full.at[u(16 * h + 4 * rem(i1 + 3, 4), 2)]
            high = self.full.at[u(16 * h + 4 * rem(i1 + 1, 4) + 2, 2)]
            self.go(8, 6, low, low, peer1(1))
            self.go(8, 6, high, high, peer1(3))

    def s8(self):
        self.got(6, self.full, 16)


def pack(source, narrow, store, groups, ends):
    def body(q, carry):
        rows = pl.ds(pl.multiple_of(q * SUB, SUB), SUB)
        for g in groups:
            store(q, g, source[rows, LANES * g : LANES * (g + 1)].astype(BF16))
        return carry

    lax.fori_loop(0, 5, body, 0)
    narrow[:, :TAIL] = source[:, LAST]
    lane = lax.broadcasted_iota(jnp.int32, (TAILROWS, LANES), 1)
    packed = jnp.where(lane < TAIL, narrow[:TAILROWS, :], pltpu.roll(narrow[TAILROWS:, :], TAIL, 1))
    blank = jnp.zeros((4 * SUB - TAILROWS, LANES), F32)
    blocks = [packed[:SUB], packed[SUB : 2 * SUB], jnp.concatenate([packed[2 * SUB :], blank[:SUB // 2]], axis=0), blank[SUB // 2 :]]
    for g in ends:
        store(5, g, blocks[g].astype(BF16))


def tail(read):
    return jnp.concatenate([read(60), read(61), read(62)[: TAILROWS - 2 * SUB]], axis=0)


def kernel(
    w_hbm, m_hbm, tok_hbm, tgt_hbm, bw_ref, avg_hbm, bl_hbm, bw_hbm, sum_hbm,
    tok, tgt, w, m, g, half, narrow, avg, bl, bw, tsend, trecv, lsem, osem, *sum_refs,
):
    rep, shard = lax.axis_index("rep"), lax.axis_index("shard")
    x, zl, y = rep // 8, rem(rep // 4, 2), rem(rep, 4)
    zh, core = shard // 2, rem(shard, 2)
    right = (rep, 2 * rem(zh + 1, 4) + core)
    left = (rep, 2 * rem(zh + 3, 4) + core)
    partner = (rep, 2 * zh + 1 - core)
    pair_id = (8 * x + 4 * (1 - zl) + y, shard)

    def along_x(d):
        return (8 * rem(x + d, 4) + 4 * zl + y, shard)

    def along_y(d):
        return (8 * x + 4 * zl + rem(y + d, 4), shard)

    place = (((x, along_x), (y, along_y)), pair_id)
    per = len(Sum.sizes) + 2
    first = Sum(sum_refs[:per], place, 2, F32)
    second = Sum(sum_refs[per : 2 * per], place, 2, BF16)
    even = Sum(sum_refs[2 * per : 3 * per], place, 1, BF16)
    odd = Sum(sum_refs[3 * per :], place, 1, BF16)

    def into(total):
        def store(q, g, block):
            total.own[GROUPS * q + g] = block

        return store

    def into_half(total):
        def store(q, g, block):
            total.own[GROUPS // 2 * q + g // 2] = block

        return store


    loads = [
        pltpu.make_async_copy(tok_hbm.at[0], tok.at[0, 0, core], lsem.at[0]),
        pltpu.make_async_copy(w_hbm, w, lsem.at[1]),
        pltpu.make_async_copy(m_hbm, m, lsem.at[2]),
        pltpu.make_async_copy(tgt_hbm, tgt, lsem.at[3]),
        pltpu.make_async_copy(tok_hbm.at[1], tok.at[1, 0, core], lsem.at[4]),
    ]
    for load in loads:
        load.start()

    peers = [right, left, partner, pair_id] + [f(d) for f in (along_x, along_y) for d in (1, 2, 3)]
    barrier = pltpu.get_barrier_semaphore()
    for peer in peers:
        pl.semaphore_signal(barrier, inc=1, device_id=peer, device_id_type=MESH)
    pl.semaphore_wait(barrier, len(peers))

    def move(step, relay, src, dst, recv, device):
        pltpu.make_async_remote_copy(
            src_ref=src,
            dst_ref=dst,
            send_sem=tsend.at[step, relay],
            recv_sem=recv,
            device_id=device,
            device_id_type=MESH,
        ).start()

    def drain(step, relay):
        everything = tok.at[step, 0, 0] if relay else tok.at[step, pl.ds(0, 3)]
        pltpu.make_async_remote_copy(
            src_ref=everything,
            dst_ref=everything,
            send_sem=tsend.at[step, relay],
            recv_sem=trecv.at[step, 0, 0, 0],
            device_id=partner,
            device_id_type=MESH,
        ).wait_send()

    def came(recv, dst):
        pltpu.make_async_remote_copy(
            src_ref=dst,
            dst_ref=dst,
            send_sem=tsend.at[0, 0],
            recv_sem=recv,
            device_id=partner,
            device_id_type=MESH,
        ).wait_recv()

    def send_own(step):
        lower, upper = tok.at[step, 0, core, 0], tok.at[step, 0, core, 1]
        for src, chip, part, device in (
            (lower, 1, 0, right), (upper, 2, 1, left), (upper, 1, 1, right), (lower, 2, 0, left),
        ):
            move(step, 0, src, tok.at[step, chip, core, part], trecv.at[step, chip, core, part], device)
        both = tok.at[step, 0, core]
        move(step, 0, both, both, trecv.at[step, 0, core, 0], partner)

    waves = {1: ((1, 0), (2, 1)), 2: ((1, 1), (2, 0)), 3: ((3, 0), (3, 1))}

    def receive(step, wave):
        for k, (chip, part) in enumerate(waves[wave]):
            here, recv = tok.at[step, chip, core, part], trecv.at[step, chip, core, part]
            came(recv, here)
            if wave == 1:
                move(step, 1, here, tok.at[step, 3, core, part], trecv.at[step, 3, core, part], (right, left)[k])
            move(step, 0, here, here, recv, partner)

    def receive_partner(step, wave):
        if wave == 0:
            came(trecv.at[step, 0, 1 - core, 0], tok.at[step, 0, 1 - core])
            return
        for chip, part in waves[wave]:
            came(trecv.at[step, chip, 1 - core, part], tok.at[step, chip, 1 - core, part])

    scaling = 1.0 / math.sqrt(D)
    root = math.sqrt(2.0 / math.pi)

    def compute(step, chip):
        block = jnp.concatenate([tok[step, chip, c].reshape(D, TOKS) for c in range(2)], axis=1)
        value = jnp.dot(half[...], block, preferred_element_type=F32) * scaling
        start = rem(zh + (0, 3, 1, 2)[chip], 4) * (2 * TOKS)
        wanted = tgt[step, :, pl.ds(pl.multiple_of(start, 2 * TOKS), 2 * TOKS)].astype(F32)
        square = value * value
        curve = jnp.tanh(root * value * (1.0 + 0.044715 * square))
        gate = 0.5 * (1.0 + curve)
        slope = gate + 0.5 * value * (1.0 - curve * curve) * (root * (1.0 + 3 * 0.044715 * square))
        grad = ((value * gate - wanted) * slope * scaling).astype(BF16)
        part = lax.dot_general(grad, block, (((1,), (1,)), ((), ())), preferred_element_type=F32)
        if chip == 0:
            g[...] = part
        else:
            g[...] += part

    share = 1.0 / REPS
    every, ends = range(GROUPS), range(4)
    loads[0].wait()
    send_own(0)
    loads[1].wait()
    half[...] = w[...].astype(BF16)
    pack(w, narrow, into(first), every, ends)
    first.s1()
    loads[2].wait()
    loads[3].wait()
    loads[4].wait()

    receive_partner(0, 0)
    compute(0, 0)
    first.s1b()
    first.s2()
    first.s3()
    first.s4()

    receive(0, 1)
    receive(0, 2)
    receive_partner(0, 1)
    receive_partner(0, 2)
    compute(0, 1)
    compute(0, 2)
    first.s5()
    drain(0, 1)
    send_own(1)

    receive(0, 3)
    first.s6()
    receive_partner(0, 3)
    compute(0, 3)
    first.s6b()
    m[...] = momentum_decay * m[...] + g[...]
    half[...] = (w[...] - learn_rate * m[...]).astype(BF16)
    pack(m, narrow, into(second), every, ends)
    second.s1()
    first.s7()

    receive_partner(1, 0)
    compute(1, 0)
    second.s1b()
    second.s2()
    second.s3()
    second.s4()

    receive(1, 1)
    receive(1, 2)
    receive_partner(1, 1)
    receive_partner(1, 2)
    compute(1, 1)
    first.s8()
    second.s5()
    compute(1, 2)
    second.s6()
    second.s6b()

    receive(1, 3)
    receive_partner(1, 3)
    compute(1, 3)
    pack(g, narrow, into_half(even), every[::2], ends[::2])
    even.s1()
    pack(g, narrow, into_half(odd), every[1::2], ends[1::2])
    even.flush()
    odd.s1()
    second.s7()
    odd.flush()
    even.s1b()
    odd.s1b()
    m[...] = momentum_decay * m[...] + g[...]
    even.s2()
    even.flush()
    odd.s2()
    second.s8()

    same = lax.broadcasted_iota(jnp.int32, (COLS, COLS), 0) == lax.broadcasted_iota(jnp.int32, (COLS, COLS), 1)
    column = jnp.sum(jnp.where(same, bw_ref[...], 0.0), axis=1, keepdims=True)
    bw[...] = jnp.broadcast_to(column, (COLS, LANES))

    def sums(block):
        w0 = first.full[block].astype(F32)
        m1 = second.full[block].astype(F32)
        average = w0 - (learn_rate * (1.0 + momentum_decay)) * m1
        return average * share, m1 * (momentum_decay * share)

    def base(q, carry):
        rows = pl.ds(pl.multiple_of(q * SUB, SUB), SUB)
        part = bw[rows, :]
        for k in range(GROUPS):
            columns = slice(LANES * k, LANES * (k + 1))
            average, mean = sums(GROUPS * q + k)
            avg[rows, columns] = average
            bl[rows, columns] = part * mean + (1.0 - part) * m[rows, columns]
        return carry

    lax.fori_loop(0, 5, base, 0)
    for b in range(2):
        rows = slice(TAILROWS * b, TAILROWS * (b + 1))
        average, mean = (tail(lambda block: sums(block)[k]) for k in range(2))
        if b:
            average, mean = pltpu.roll(average, TAIL, 1), pltpu.roll(mean, TAIL, 1)
        part = bw[rows, :TAIL]
        avg[rows, LAST] = average[:, :TAIL]
        bl[rows, LAST] = part * mean[:, :TAIL] + (1.0 - part) * m[rows, LAST]
    outs = [
        pltpu.make_async_copy(avg, avg_hbm, lsem.at[0]),
        pltpu.make_async_copy(bl, bl_hbm, lsem.at[1]),
        pltpu.make_async_copy(bw, bw_hbm, lsem.at[2]),
    ]
    for out in outs:
        out.start()

    even.s3()
    even.flush()
    odd.s3()
    even.s4()
    even.flush()
    odd.s4()
    even.s5()
    even.flush()
    odd.s5()
    even.s6()
    even.flush()
    odd.s6()
    odd.flush()
    even.s6b()
    odd.s6b()
    even.s7()
    odd.s7()
    even.s8()

    def store(k, total):
        for part in range(4):
            here = pl.ds(8 * part, 8)
            outs.append(pltpu.make_async_copy(total.full.at[here], sum_hbm.at[k, here], osem.at[k, part]))
            outs[-1].start()

    store(0, even)
    odd.s8()
    store(1, odd)
    def end_sends():
        drain(0, 0)
        drain(1, 0)
        drain(1, 1)
        for total in (first, second, even, odd):
            total.flush()

    def end_outs():
        for out in outs:
            out.wait()

    end_sends()
    end_outs()


def finish(avg_hbm, bl_hbm, bw_hbm, sum_hbm, avg_out, bl_out, avg, bl, bw, total, sem):
    rows = [pl.ds(SUB * q, SUB) for q in range(5)]
    small = [
        pltpu.make_async_copy(sum_hbm.at[:, pl.ds(30, 2)], total.at[:, pl.ds(30, 2)], sem.at[0]),
        pltpu.make_async_copy(bw_hbm, bw, sem.at[1]),
    ]
    loads = [
        [
            pltpu.make_async_copy(sum_hbm.at[:, pl.ds(6 * q, 6)], total.at[:, pl.ds(6 * q, 6)], sem.at[2 + q]),
            pltpu.make_async_copy(avg_hbm.at[rows[q]], avg.at[rows[q]], sem.at[7 + q]),
            pltpu.make_async_copy(bl_hbm.at[rows[q]], bl.at[rows[q]], sem.at[12 + q]),
        ]
        for q in range(5)
    ]
    for copy in small + sum(loads, []):
        copy.start()
    share = 1.0 / REPS
    for copy in small:
        copy.wait()
    ends = [tail(lambda block: total[block % 2, block // 2].astype(F32)) * share]
    ends.append(pltpu.roll(ends[0], TAIL, 1))
    outs = []
    for q in range(5):
        for copy in loads[q]:
            copy.wait()
        part = bw[rows[q], :] * share
        for k in range(GROUPS):
            columns = slice(LANES * k, LANES * (k + 1))
            value = total[k % 2, 6 * q + k // 2].astype(F32)
            avg[rows[q], columns] = avg[rows[q], columns] - (learn_rate * share) * value
            bl[rows[q], columns] = bl[rows[q], columns] + part * value
        for b in range(2):
            start, stop = max(SUB * q, TAILROWS * b), min(SUB * (q + 1), TAILROWS * (b + 1))
            if start < stop:
                here = slice(start, stop)
                value = ends[b][start - TAILROWS * b : stop - TAILROWS * b, :TAIL]
                avg[here, LAST] = avg[here, LAST] - learn_rate * value
                bl[here, LAST] = bl[here, LAST] + bw[here, :TAIL] * value
        for source, out, slot in ((avg, avg_out, 17 + q), (bl, bl_out, 22 + q)):
            outs.append(pltpu.make_async_copy(source.at[rows[q]], out.at[rows[q]], sem.at[slot]))
            outs[-1].start()
    for out in outs:
        out.wait()


def local(params, momentum, tokens, targets, blend_weight):
    anywhere = pl.BlockSpec(memory_space=pl.ANY)
    whole = jax.ShapeDtypeStruct((COLS, D), F32)
    parts = pl.pallas_call(
        kernel,
        out_shape=[
            whole,
            whole,
            jax.ShapeDtypeStruct((COLS, LANES), F32),
            jax.ShapeDtypeStruct((2, 32, SUB, LANES), BF16),
        ],
        in_specs=[anywhere] * 4 + [pl.BlockSpec(memory_space=pltpu.VMEM)],
        out_specs=[anywhere] * 4,
        scratch_shapes=[
            pltpu.VMEM((2, 4, 2, 2, D // 2, TOKS), BF16),
            pltpu.VMEM((2, COLS, 1024), BF16),
            pltpu.VMEM((COLS, D), F32),
            pltpu.VMEM((COLS, D), F32),
            pltpu.VMEM((COLS, D), F32),
            pltpu.VMEM((COLS, D), BF16),
            pltpu.VMEM((COLS, LANES), F32),
            pltpu.VMEM((COLS, D), F32),
            pltpu.VMEM((COLS, D), F32),
            pltpu.VMEM((COLS, LANES), F32),
            pltpu.SemaphoreType.DMA((2, 2)),
            pltpu.SemaphoreType.DMA((2, 4, 2, 2)),
            pltpu.SemaphoreType.DMA((5,)),
            pltpu.SemaphoreType.DMA((2, 4)),
            *Sum.scratch(2, F32),
            *Sum.scratch(2, BF16),
            *Sum.scratch(1, BF16),
            *Sum.scratch(1, BF16),
        ],
        compiler_params=pltpu.CompilerParams(
            collective_id=0, has_side_effects=True, vmem_limit_bytes=67043328
        ),
        name="window",
    )(
        params[0].T,
        momentum[0].T,
        tokens[0].transpose(0, 2, 1).reshape(2, 2, D // 2, TOKS),
        targets[0].transpose(0, 2, 1),
        blend_weight.reshape(1, COLS),
    )
    averaged, blended = pl.pallas_call(
        finish,
        out_shape=[whole, whole],
        in_specs=[anywhere] * 4,
        out_specs=[anywhere] * 2,
        scratch_shapes=[
            pltpu.VMEM((COLS, D), F32),
            pltpu.VMEM((COLS, D), F32),
            pltpu.VMEM((COLS, LANES), F32),
            pltpu.VMEM((2, 32, SUB, LANES), BF16),
            pltpu.SemaphoreType.DMA((27,)),
        ],
        name="finish",
    )(*parts)
    return averaged.T, blended.T[None]


def solution(mesh):
    return jax.shard_map(
        local,
        mesh=mesh,
        in_specs=(
            P("rep", None, "shard"),
            P("rep", None, "shard"),
            P("rep", None, "shard", None),
            P("rep", None, None, "shard"),
            P("shard"),
        ),
        out_specs=(P(None, "shard"), P("rep", None, "shard")),
        check_vma=False,
    )
```

```python
import functools
import math

import jax
import jax.numpy as jnp
from jax import lax
from jax.experimental import pallas as pl
from jax.experimental.pallas import tpu as pltpu
from jax.sharding import PartitionSpec as P

D = 1600
COLS = 400
REPS = 32
LANES = 128
SUB = 80
GROUPS = 12
TAIL = 64
TAILROWS = 200
TOKS = 128

learn_rate = 0.05
momentum_decay = 0.9

MESH = pl.DeviceIdType.MESH
F32 = jnp.float32
BF16 = jnp.bfloat16
LAST = slice(GROUPS * LANES, D)


def rem(value, count):
    return lax.rem(value, jnp.int32(count))


class Sum:
    sizes = dict(own=32, far=8, mid=8, near=16, part=8, cross=6, pair=2, other=2, full=32)

    def __init__(self, refs, place, per, wide):
        self.flight = []
        self.per = per
        names = list(self.sizes)
        for name, ref in zip(names, refs[: len(names)]):
            setattr(self, name, ref)
        self.send, self.recv = refs[len(names) :]
        self.wide = wide
        self.rings, self.pair_id = place

    @classmethod
    def scratch(cls, per, wide):
        inner = ("part", "cross")
        return [
            pltpu.VMEM((per * n, SUB, LANES), wide if name in inner else BF16) for name, n in cls.sizes.items()
        ] + [pltpu.SemaphoreType.DMA((9,)), pltpu.SemaphoreType.DMA((7,))]

    def units(self, first, count):
        return pl.ds(self.per * first, self.per * count)

    def copy(self, stage, kind, src, dst, device):
        return pltpu.make_async_remote_copy(
            src_ref=src,
            dst_ref=dst,
            send_sem=self.send.at[stage],
            recv_sem=self.recv.at[kind],
            device_id=device,
            device_id_type=MESH,
        )

    def go(self, stage, kind, src, dst, device):
        self.copy(stage, kind, src, dst, device).start()
        if stage not in self.flight:
            self.flight.append(stage)

    def flush(self):
        for stage in self.flight:
            source, count = ((self.own, 8), (self.own, 8), (self.mid, 8), (self.part, 6), (self.pair, 2), (self.full, 6), (self.full, 8), (self.full, 8), (self.full, 8))[stage]
            all_sent = source.at[self.units(0, count)]
            self.copy(stage, 0, all_sent, all_sent, self.pair_id).wait_send()
        self.flight = []

    def got(self, kind, ref, count):
        everything = ref.at[self.units(0, count)]
        self.copy(0, kind, everything, everything, self.pair_id).wait_recv()

    def halves(self):
        for h in range(2):
            (i1, peer1), (i2, peer2) = self.rings if h == 0 else self.rings[::-1]
            yield h, i1, peer1, i2, peer2

    def s1(self):
        u = self.units
        for h, i1, peer1, i2, peer2 in self.halves():
            base = 16 * h + 4 * rem(i1 + 2, 4)
            self.go(0, 0, self.own.at[u(base, 2)], self.far.at[u(4 * h, 2)], peer1(1))
            self.go(0, 0, self.own.at[u(base + 2, 2)], self.far.at[u(4 * h + 2, 2)], peer1(3))

    def s1b(self):
        u = self.units
        for h, i1, peer1, i2, peer2 in self.halves():
            right = 16 * h + 4 * rem(i1 + 1, 4)
            left = 16 * h + 4 * rem(i1 + 3, 4)
            self.go(1, 1, self.own.at[u(right + 2, 2)], self.near.at[u(8 * h + 2, 2)], peer1(1))
            self.go(1, 1, self.own.at[u(left, 2)], self.near.at[u(8 * h + 4, 2)], peer1(3))

    def s2(self):
        u = self.units
        self.got(0, self.far, 8)
        for h, i1, peer1, i2, peer2 in self.halves():
            right = 16 * h + 4 * rem(i1 + 1, 4)
            left = 16 * h + 4 * rem(i1 + 3, 4)
            for side, first, at in ((0, right, 0), (1, left + 2, 6)):
                here = u(4 * h + 2 * side, 2)
                self.mid[here] = (self.own[u(first, 2)].astype(F32) + self.far[here].astype(F32)).astype(BF16)
                self.go(2, 1, self.mid.at[here], self.near.at[u(8 * h + at, 2)], peer1(1 + 2 * side))

    def s3(self):
        u = self.units
        self.got(1, self.near, 16)
        for h, i1, peer1, i2, peer2 in self.halves():
            mine = 16 * h + 4 * i1
            self.part[u(4 * h, 4)] = (
                self.own[u(mine, 4)].astype(F32)
                + self.near[u(8 * h, 4)].astype(F32)
                + self.near[u(8 * h + 4, 4)].astype(F32)
            ).astype(self.wide)
            for d in range(1, 4):
                self.go(
                    3, 2, self.part.at[u(4 * h + rem(i2 + d, 4), 1)], self.cross.at[u(3 * h + d - 1, 1)], peer2(d)
                )

    def s4(self):
        u = self.units
        self.got(2, self.cross, 6)
        for h, i1, peer1, i2, peer2 in self.halves():
            total = self.part[u(4 * h + i2, 1)].astype(F32)
            for d in range(1, 4):
                total = total + self.cross[u(3 * h + d - 1, 1)].astype(F32)
            self.pair[u(h, 1)] = total.astype(BF16)
            self.go(4, 3, self.pair.at[u(h, 1)], self.other.at[u(h, 1)], self.pair_id)

    def s5(self):
        u = self.units
        self.got(3, self.other, 2)
        for h, i1, peer1, i2, peer2 in self.halves():
            mine = u(16 * h + 4 * i1 + i2, 1)
            self.full[mine] = (self.pair[u(h, 1)].astype(F32) + self.other[u(h, 1)].astype(F32)).astype(BF16)
            for d in range(1, 4):
                self.go(5, 4, self.full.at[mine], self.full.at[mine], peer2(d))

    def sides(self):
        for h, i1, peer1, i2, peer2 in self.halves():
            low, high = (self.full.at[self.units(16 * h + 4 * i1 + at, 2)] for at in (0, 2))
            yield low, high, peer1

    def s6(self):
        self.got(4, self.full, 6)
        for low, high, peer1 in self.sides():
            self.go(6, 5, low, low, peer1(1))
            self.go(6, 5, high, high, peer1(3))

    def s6b(self):
        for low, high, peer1 in self.sides():
            self.go(7, 6, high, high, peer1(1))
            self.go(7, 6, low, low, peer1(3))

    def s7(self):
        u = self.units
        self.got(5, self.full, 8)
        for h, i1, peer1, i2, peer2 in self.halves():
            low = self.full.at[u(16 * h + 4 * rem(i1 + 3, 4), 2)]
            high = self.full.at[u(16 * h + 4 * rem(i1 + 1, 4) + 2, 2)]
            self.go(8, 6, low, low, peer1(1))
            self.go(8, 6, high, high, peer1(3))

    def s8(self):
        self.got(6, self.full, 16)


def pack(source, narrow, store, groups, ends):
    def body(q, carry):
        rows = pl.ds(pl.multiple_of(q * SUB, SUB), SUB)
        for g in groups:
            store(q, g, source[rows, LANES * g : LANES * (g + 1)].astype(BF16))
        return carry

    lax.fori_loop(0, 5, body, 0)
    narrow[:, :TAIL] = source[:, LAST]
    lane = lax.broadcasted_iota(jnp.int32, (TAILROWS, LANES), 1)
    packed = jnp.where(lane < TAIL, narrow[:TAILROWS, :], pltpu.roll(narrow[TAILROWS:, :], TAIL, 1))
    blank = jnp.zeros((4 * SUB - TAILROWS, LANES), F32)
    blocks = [packed[:SUB], packed[SUB : 2 * SUB], jnp.concatenate([packed[2 * SUB :], blank[:SUB // 2]], axis=0), blank[SUB // 2 :]]
    for g in ends:
        store(5, g, blocks[g].astype(BF16))


def tail(read):
    return jnp.concatenate([read(60), read(61), read(62)[: TAILROWS - 2 * SUB]], axis=0)


def kernel(
    w_hbm, m_hbm, tok_hbm, tgt_hbm, bw_ref, avg_hbm, bl_hbm, bw_hbm, sum_hbm,
    tok, tgt, w, m, g, half, narrow, avg, bl, bw, tsend, trecv, lsem, osem, *sum_refs,
):
    rep, shard = lax.axis_index("rep"), lax.axis_index("shard")
    x, zl, y = rep // 8, rem(rep // 4, 2), rem(rep, 4)
    zh, core = shard // 2, rem(shard, 2)
    right = (rep, 2 * rem(zh + 1, 4) + core)
    left = (rep, 2 * rem(zh + 3, 4) + core)
    partner = (rep, 2 * zh + 1 - core)
    pair_id = (8 * x + 4 * (1 - zl) + y, shard)

    def along_x(d):
        return (8 * rem(x + d, 4) + 4 * zl + y, shard)

    def along_y(d):
        return (8 * x + 4 * zl + rem(y + d, 4), shard)

    place = (((x, along_x), (y, along_y)), pair_id)
    per = len(Sum.sizes) + 2
    first = Sum(sum_refs[:per], place, 2, F32)
    second = Sum(sum_refs[per : 2 * per], place, 2, BF16)
    even = Sum(sum_refs[2 * per : 3 * per], place, 1, BF16)
    odd = Sum(sum_refs[3 * per :], place, 1, BF16)

    def into(total):
        def store(q, g, block):
            total.own[GROUPS * q + g] = block

        return store

    def into_half(total):
        def store(q, g, block):
            total.own[GROUPS // 2 * q + g // 2] = block

        return store


    loads = [
        pltpu.make_async_copy(tok_hbm.at[0], tok.at[0, 0, core], lsem.at[0]),
        pltpu.make_async_copy(w_hbm, w, lsem.at[1]),
        pltpu.make_async_copy(m_hbm, m, lsem.at[2]),
        pltpu.make_async_copy(tgt_hbm, tgt, lsem.at[3]),
        pltpu.make_async_copy(tok_hbm.at[1], tok.at[1, 0, core], lsem.at[4]),
    ]
    for load in loads:
        load.start()

    peers = [right, left, partner, pair_id] + [f(d) for f in (along_x, along_y) for d in (1, 2, 3)]
    barrier = pltpu.get_barrier_semaphore()
    for peer in peers:
        pl.semaphore_signal(barrier, inc=1, device_id=peer, device_id_type=MESH)
    pl.semaphore_wait(barrier, len(peers))

    def move(step, relay, src, dst, recv, device):
        pltpu.make_async_remote_copy(
            src_ref=src,
            dst_ref=dst,
            send_sem=tsend.at[step, relay],
            recv_sem=recv,
            device_id=device,
            device_id_type=MESH,
        ).start()

    def drain(step, relay):
        everything = tok.at[step, 0, 0] if relay else tok.at[step, pl.ds(0, 3)]
        pltpu.make_async_remote_copy(
            src_ref=everything,
            dst_ref=everything,
            send_sem=tsend.at[step, relay],
            recv_sem=trecv.at[step, 0, 0, 0],
            device_id=partner,
            device_id_type=MESH,
        ).wait_send()

    def came(recv, dst):
        pltpu.make_async_remote_copy(
            src_ref=dst,
            dst_ref=dst,
            send_sem=tsend.at[0, 0],
            recv_sem=recv,
            device_id=partner,
            device_id_type=MESH,
        ).wait_recv()

    def send_own(step, turn):
        lower, upper = tok.at[step, 0, core, 0], tok.at[step, 0, core, 1]
        turns = (((lower, 1, 0, right), (upper, 2, 1, left)), ((upper, 1, 1, right), (lower, 2, 0, left)))
        for src, chip, part, device in turns[turn]:
            move(step, 0, src, tok.at[step, chip, core, part], trecv.at[step, chip, core, part], device)
        if turn == 0:
            both = tok.at[step, 0, core]
            move(step, 0, both, both, trecv.at[step, 0, core, 0], partner)

    waves = {1: ((1, 0), (2, 1)), 2: ((1, 1), (2, 0)), 3: ((3, 0), (3, 1))}

    def receive(step, wave):
        for k, (chip, part) in enumerate(waves[wave]):
            here, recv = tok.at[step, chip, core, part], trecv.at[step, chip, core, part]
            came(recv, here)
            if wave == 1:
                move(step, 1, here, tok.at[step, 3, core, part], trecv.at[step, 3, core, part], (right, left)[k])
            move(step, 0, here, here, recv, partner)

    def receive_partner(step, wave):
        if wave == 0:
            came(trecv.at[step, 0, 1 - core, 0], tok.at[step, 0, 1 - core])
            return
        for chip, part in waves[wave]:
            came(trecv.at[step, chip, 1 - core, part], tok.at[step, chip, 1 - core, part])

    scaling = 1.0 / math.sqrt(D)
    root = math.sqrt(2.0 / math.pi)

    def compute(step, chip):
        block = jnp.concatenate([tok[step, chip, c].reshape(D, TOKS) for c in range(2)], axis=1)
        value = jnp.dot(half[...], block, preferred_element_type=F32) * scaling
        start = rem(zh + (0, 3, 1, 2)[chip], 4) * (2 * TOKS)
        wanted = tgt[step, :, pl.ds(pl.multiple_of(start, 2 * TOKS), 2 * TOKS)].astype(F32)
        square = value * value
        curve = jnp.tanh(root * value * (1.0 + 0.044715 * square))
        gate = 0.5 * (1.0 + curve)
        slope = gate + 0.5 * value * (1.0 - curve * curve) * (root * (1.0 + 3 * 0.044715 * square))
        grad = ((value * gate - wanted) * slope * scaling).astype(BF16)
        part = lax.dot_general(grad, block, (((1,), (1,)), ((), ())), preferred_element_type=F32)
        if chip == 0:
            g[...] = part
        else:
            g[...] += part

    share = 1.0 / REPS
    every, ends = range(GROUPS), range(4)
    loads[0].wait()
    send_own(0, 0)
    loads[1].wait()
    half[...] = w[...].astype(BF16)
    pack(w, narrow, into(first), every, ends)
    first.s1()
    loads[2].wait()
    loads[3].wait()
    loads[4].wait()

    receive_partner(0, 0)
    send_own(0, 1)
    first.s1b()
    compute(0, 0)
    first.s2()
    first.s3()

    receive(0, 1)
    first.s4()
    receive(0, 2)
    receive_partner(0, 1)
    receive_partner(0, 2)
    compute(0, 1)
    compute(0, 2)
    drain(0, 1)
    send_own(1, 0)
    first.s5()

    receive(0, 3)
    receive_partner(0, 3)
    compute(0, 3)
    send_own(1, 1)
    m[...] = momentum_decay * m[...] + g[...]
    half[...] = (w[...] - learn_rate * m[...]).astype(BF16)
    pack(m, narrow, into(second), every, ends)
    second.s1()

    receive_partner(1, 0)
    compute(1, 0)
    second.s1b()
    second.s2()
    second.s3()

    receive(1, 1)
    first.s6()
    first.s6b()
    second.s4()
    receive(1, 2)
    first.s7()
    receive_partner(1, 1)
    receive_partner(1, 2)
    compute(1, 1)
    compute(1, 2)

    receive(1, 3)
    second.s5()
    receive_partner(1, 3)
    compute(1, 3)
    pack(g, narrow, into_half(even), every[::2], ends[::2])
    even.s1()
    pack(g, narrow, into_half(odd), every[1::2], ends[1::2])
    even.flush()
    odd.s1()
    odd.flush()
    even.s1b()
    odd.s1b()
    m[...] = momentum_decay * m[...] + g[...]
    even.s2()
    even.flush()
    odd.s2()
    even.s3()
    odd.s3()
    second.s6()
    second.s6b()
    even.s4()
    odd.s4()
    even.s5()
    odd.s5()
    second.s7()
    even.s6()
    even.flush()
    odd.s6()
    odd.flush()
    even.s6b()
    odd.s6b()
    first.s8()
    second.s8()

    same = lax.broadcasted_iota(jnp.int32, (COLS, COLS), 0) == lax.broadcasted_iota(jnp.int32, (COLS, COLS), 1)
    column = jnp.sum(jnp.where(same, bw_ref[...], 0.0), axis=1, keepdims=True)
    bw[...] = jnp.broadcast_to(column, (COLS, LANES))

    def sums(block):
        w0 = first.full[block].astype(F32)
        m1 = second.full[block].astype(F32)
        average = w0 - (learn_rate * (1.0 + momentum_decay)) * m1
        return average * share, m1 * (momentum_decay * share)

    def base(q, carry):
        rows = pl.ds(pl.multiple_of(q * SUB, SUB), SUB)
        part = bw[rows, :]
        for k in range(GROUPS):
            columns = slice(LANES * k, LANES * (k + 1))
            average, mean = sums(GROUPS * q + k)
            avg[rows, columns] = average
            bl[rows, columns] = part * mean + (1.0 - part) * m[rows, columns]
        return carry

    lax.fori_loop(0, 5, base, 0)
    for b in range(2):
        rows = slice(TAILROWS * b, TAILROWS * (b + 1))
        average, mean = (tail(lambda block: sums(block)[k]) for k in range(2))
        if b:
            average, mean = pltpu.roll(average, TAIL, 1), pltpu.roll(mean, TAIL, 1)
        part = bw[rows, :TAIL]
        avg[rows, LAST] = average[:, :TAIL]
        bl[rows, LAST] = part * mean[:, :TAIL] + (1.0 - part) * m[rows, LAST]
    outs = [
        pltpu.make_async_copy(avg, avg_hbm, lsem.at[0]),
        pltpu.make_async_copy(bl, bl_hbm, lsem.at[1]),
        pltpu.make_async_copy(bw, bw_hbm, lsem.at[2]),
    ]
    for out in outs:
        out.start()

    even.s7()
    odd.s7()
    even.s8()

    def store(k, total):
        for part in range(4):
            here = pl.ds(8 * part, 8)
            outs.append(pltpu.make_async_copy(total.full.at[here], sum_hbm.at[k, here], osem.at[k, part]))
            outs[-1].start()

    store(0, even)
    odd.s8()
    store(1, odd)
    def end_sends():
        drain(0, 0)
        drain(1, 0)
        drain(1, 1)
        for total in (first, second, even, odd):
            total.flush()

    def end_outs():
        for out in outs:
            out.wait()

    end_sends()
    end_outs()


def finish(avg_hbm, bl_hbm, bw_hbm, sum_hbm, avg_out, bl_out, avg, bl, bw, total, sem):
    rows = [pl.ds(SUB * q, SUB) for q in range(5)]
    small = [
        pltpu.make_async_copy(sum_hbm.at[:, pl.ds(30, 2)], total.at[:, pl.ds(30, 2)], sem.at[0]),
        pltpu.make_async_copy(bw_hbm, bw, sem.at[1]),
    ]
    loads = [
        [
            pltpu.make_async_copy(sum_hbm.at[:, pl.ds(6 * q, 6)], total.at[:, pl.ds(6 * q, 6)], sem.at[2 + q]),
            pltpu.make_async_copy(avg_hbm.at[rows[q]], avg.at[rows[q]], sem.at[7 + q]),
            pltpu.make_async_copy(bl_hbm.at[rows[q]], bl.at[rows[q]], sem.at[12 + q]),
        ]
        for q in range(5)
    ]
    for copy in small + sum(loads, []):
        copy.start()
    share = 1.0 / REPS
    for copy in small:
        copy.wait()
    ends = [tail(lambda block: total[block % 2, block // 2].astype(F32)) * share]
    ends.append(pltpu.roll(ends[0], TAIL, 1))
    outs = []
    for q in range(5):
        for copy in loads[q]:
            copy.wait()
        part = bw[rows[q], :] * share
        for k in range(GROUPS):
            columns = slice(LANES * k, LANES * (k + 1))
            value = total[k % 2, 6 * q + k // 2].astype(F32)
            avg[rows[q], columns] = avg[rows[q], columns] - (learn_rate * share) * value
            bl[rows[q], columns] = bl[rows[q], columns] + part * value
        for b in range(2):
            start, stop = max(SUB * q, TAILROWS * b), min(SUB * (q + 1), TAILROWS * (b + 1))
            if start < stop:
                here = slice(start, stop)
                value = ends[b][start - TAILROWS * b : stop - TAILROWS * b, :TAIL]
                avg[here, LAST] = avg[here, LAST] - learn_rate * value
                bl[here, LAST] = bl[here, LAST] + bw[here, :TAIL] * value
        for source, out, slot in ((avg, avg_out, 17 + q), (bl, bl_out, 22 + q)):
            outs.append(pltpu.make_async_copy(source.at[rows[q]], out.at[rows[q]], sem.at[slot]))
            outs[-1].start()
    for out in outs:
        out.wait()


def local(params, momentum, tokens, targets, blend_weight):
    anywhere = pl.BlockSpec(memory_space=pl.ANY)
    whole = jax.ShapeDtypeStruct((COLS, D), F32)
    parts = pl.pallas_call(
        kernel,
        out_shape=[
            whole,
            whole,
            jax.ShapeDtypeStruct((COLS, LANES), F32),
            jax.ShapeDtypeStruct((2, 32, SUB, LANES), BF16),
        ],
        in_specs=[anywhere] * 4 + [pl.BlockSpec(memory_space=pltpu.VMEM)],
        out_specs=[anywhere] * 4,
        scratch_shapes=[
            pltpu.VMEM((2, 4, 2, 2, D // 2, TOKS), BF16),
            pltpu.VMEM((2, COLS, 1024), BF16),
            pltpu.VMEM((COLS, D), F32),
            pltpu.VMEM((COLS, D), F32),
            pltpu.VMEM((COLS, D), F32),
            pltpu.VMEM((COLS, D), BF16),
            pltpu.VMEM((COLS, LANES), F32),
            pltpu.VMEM((COLS, D), F32),
            pltpu.VMEM((COLS, D), F32),
            pltpu.VMEM((COLS, LANES), F32),
            pltpu.SemaphoreType.DMA((2, 2)),
            pltpu.SemaphoreType.DMA((2, 4, 2, 2)),
            pltpu.SemaphoreType.DMA((5,)),
            pltpu.SemaphoreType.DMA((2, 4)),
            *Sum.scratch(2, F32),
            *Sum.scratch(2, BF16),
            *Sum.scratch(1, BF16),
            *Sum.scratch(1, BF16),
        ],
        compiler_params=pltpu.CompilerParams(
            collective_id=0, has_side_effects=True, vmem_limit_bytes=67043328
        ),
        name="window",
    )(
        params[0].T,
        momentum[0].T,
        tokens[0].transpose(0, 2, 1).reshape(2, 2, D // 2, TOKS),
        targets[0].transpose(0, 2, 1),
        blend_weight.reshape(1, COLS),
    )
    averaged, blended = pl.pallas_call(
        finish,
        out_shape=[whole, whole],
        in_specs=[anywhere] * 4,
        out_specs=[anywhere] * 2,
        scratch_shapes=[
            pltpu.VMEM((COLS, D), F32),
            pltpu.VMEM((COLS, D), F32),
            pltpu.VMEM((COLS, LANES), F32),
            pltpu.VMEM((2, 32, SUB, LANES), BF16),
            pltpu.SemaphoreType.DMA((27,)),
        ],
        name="finish",
    )(*parts)
    return averaged.T, blended.T[None]


def solution(mesh):
    return jax.shard_map(
        local,
        mesh=mesh,
        in_specs=(
            P("rep", None, "shard"),
            P("rep", None, "shard"),
            P("rep", None, "shard", None),
            P("rep", None, None, "shard"),
            P("shard"),
        ),
        out_specs=(P(None, "shard"), P("rep", None, "shard")),
        check_vma=False,
    )
```

```python
import functools
import math

import jax
import jax.numpy as jnp
from jax import lax
from jax.experimental import pallas as pl
from jax.experimental.pallas import tpu as pltpu
from jax.sharding import PartitionSpec as P

D = 1600
COLS = 400
REPS = 32
LANES = 128
SUB = 80
GROUPS = 12
TAIL = 64
TAILROWS = 200
TOKS = 128

learn_rate = 0.05
momentum_decay = 0.9

MESH = pl.DeviceIdType.MESH
F32 = jnp.float32
BF16 = jnp.bfloat16
LAST = slice(GROUPS * LANES, D)


def rem(value, count):
    return lax.rem(value, jnp.int32(count))


class Sum:
    sizes = dict(own=32, far=8, mid=8, near=16, part=8, cross=6, pair=2, other=2, full=32)

    def __init__(self, refs, place, per, wide):
        self.flight = []
        self.per = per
        names = list(self.sizes)
        for name, ref in zip(names, refs[: len(names)]):
            setattr(self, name, ref)
        self.send, self.recv = refs[len(names) :]
        self.wide = wide
        self.rings, self.pair_id = place

    @classmethod
    def scratch(cls, per, wide):
        inner = ("part", "cross")
        return [
            pltpu.VMEM((per * n, SUB, LANES), wide if name in inner else BF16) for name, n in cls.sizes.items()
        ] + [pltpu.SemaphoreType.DMA((9,)), pltpu.SemaphoreType.DMA((7,))]

    def units(self, first, count):
        return pl.ds(self.per * first, self.per * count)

    def copy(self, stage, kind, src, dst, device):
        return pltpu.make_async_remote_copy(
            src_ref=src,
            dst_ref=dst,
            send_sem=self.send.at[stage],
            recv_sem=self.recv.at[kind],
            device_id=device,
            device_id_type=MESH,
        )

    def go(self, stage, kind, src, dst, device):
        self.copy(stage, kind, src, dst, device).start()
        if stage not in self.flight:
            self.flight.append(stage)

    def flush(self):
        for stage in self.flight:
            source, count = ((self.own, 8), (self.own, 8), (self.mid, 8), (self.part, 6), (self.pair, 2), (self.full, 6), (self.full, 8), (self.full, 8), (self.full, 8))[stage]
            all_sent = source.at[self.units(0, count)]
            self.copy(stage, 0, all_sent, all_sent, self.pair_id).wait_send()
        self.flight = []

    def got(self, kind, ref, count):
        everything = ref.at[self.units(0, count)]
        self.copy(0, kind, everything, everything, self.pair_id).wait_recv()

    def halves(self):
        for h in range(2):
            (i1, peer1), (i2, peer2) = self.rings if h == 0 else self.rings[::-1]
            yield h, i1, peer1, i2, peer2

    def s1(self):
        u = self.units
        for h, i1, peer1, i2, peer2 in self.halves():
            base = 16 * h + 4 * rem(i1 + 2, 4)
            self.go(0, 0, self.own.at[u(base, 2)], self.far.at[u(4 * h, 2)], peer1(1))
            self.go(0, 0, self.own.at[u(base + 2, 2)], self.far.at[u(4 * h + 2, 2)], peer1(3))

    def s1b(self):
        u = self.units
        for h, i1, peer1, i2, peer2 in self.halves():
            right = 16 * h + 4 * rem(i1 + 1, 4)
            left = 16 * h + 4 * rem(i1 + 3, 4)
            self.go(1, 1, self.own.at[u(right + 2, 2)], self.near.at[u(8 * h + 2, 2)], peer1(1))
            self.go(1, 1, self.own.at[u(left, 2)], self.near.at[u(8 * h + 4, 2)], peer1(3))

    def s2(self):
        u = self.units
        self.got(0, self.far, 8)
        for h, i1, peer1, i2, peer2 in self.halves():
            right = 16 * h + 4 * rem(i1 + 1, 4)
            left = 16 * h + 4 * rem(i1 + 3, 4)
            for side, first, at in ((0, right, 0), (1, left + 2, 6)):
                here = u(4 * h + 2 * side, 2)
                self.mid[here] = (self.own[u(first, 2)].astype(F32) + self.far[here].astype(F32)).astype(BF16)
                self.go(2, 1, self.mid.at[here], self.near.at[u(8 * h + at, 2)], peer1(1 + 2 * side))

    def s3(self):
        u = self.units
        self.got(1, self.near, 16)
        for h, i1, peer1, i2, peer2 in self.halves():
            mine = 16 * h + 4 * i1
            self.part[u(4 * h, 4)] = (
                self.own[u(mine, 4)].astype(F32)
                + self.near[u(8 * h, 4)].astype(F32)
                + self.near[u(8 * h + 4, 4)].astype(F32)
            ).astype(self.wide)
            for d in range(1, 4):
                self.go(
                    3, 2, self.part.at[u(4 * h + rem(i2 + d, 4), 1)], self.cross.at[u(3 * h + d - 1, 1)], peer2(d)
                )

    def s4(self):
        u = self.units
        self.got(2, self.cross, 6)
        for h, i1, peer1, i2, peer2 in self.halves():
            total = self.part[u(4 * h + i2, 1)].astype(F32)
            for d in range(1, 4):
                total = total + self.cross[u(3 * h + d - 1, 1)].astype(F32)
            self.pair[u(h, 1)] = total.astype(BF16)
            self.go(4, 3, self.pair.at[u(h, 1)], self.other.at[u(h, 1)], self.pair_id)

    def s5(self):
        u = self.units
        self.got(3, self.other, 2)
        for h, i1, peer1, i2, peer2 in self.halves():
            mine = u(16 * h + 4 * i1 + i2, 1)
            self.full[mine] = (self.pair[u(h, 1)].astype(F32) + self.other[u(h, 1)].astype(F32)).astype(BF16)
            for d in range(1, 4):
                self.go(5, 4, self.full.at[mine], self.full.at[mine], peer2(d))

    def sides(self):
        for h, i1, peer1, i2, peer2 in self.halves():
            low, high = (self.full.at[self.units(16 * h + 4 * i1 + at, 2)] for at in (0, 2))
            yield low, high, peer1

    def s6(self):
        self.got(4, self.full, 6)
        for low, high, peer1 in self.sides():
            self.go(6, 5, low, low, peer1(1))
            self.go(6, 5, high, high, peer1(3))

    def s6b(self):
        for low, high, peer1 in self.sides():
            self.go(7, 6, high, high, peer1(1))
            self.go(7, 6, low, low, peer1(3))

    def s7(self):
        u = self.units
        self.got(5, self.full, 8)
        for h, i1, peer1, i2, peer2 in self.halves():
            low = self.full.at[u(16 * h + 4 * rem(i1 + 3, 4), 2)]
            high = self.full.at[u(16 * h + 4 * rem(i1 + 1, 4) + 2, 2)]
            self.go(8, 6, low, low, peer1(1))
            self.go(8, 6, high, high, peer1(3))

    def s8(self):
        self.got(6, self.full, 16)


def pack(source, narrow, store, groups, ends):
    def body(q, carry):
        rows = pl.ds(pl.multiple_of(q * SUB, SUB), SUB)
        for g in groups:
            store(q, g, source[rows, LANES * g : LANES * (g + 1)].astype(BF16))
        return carry

    lax.fori_loop(0, 5, body, 0)
    narrow[:, :TAIL] = source[:, LAST]
    lane = lax.broadcasted_iota(jnp.int32, (TAILROWS, LANES), 1)
    packed = jnp.where(lane < TAIL, narrow[:TAILROWS, :], pltpu.roll(narrow[TAILROWS:, :], TAIL, 1))
    blank = jnp.zeros((4 * SUB - TAILROWS, LANES), F32)
    blocks = [packed[:SUB], packed[SUB : 2 * SUB], jnp.concatenate([packed[2 * SUB :], blank[:SUB // 2]], axis=0), blank[SUB // 2 :]]
    for g in ends:
        store(5, g, blocks[g].astype(BF16))


def tail(read):
    return jnp.concatenate([read(60), read(61), read(62)[: TAILROWS - 2 * SUB]], axis=0)


def kernel(
    w_hbm, m_hbm, tok_hbm, tgt_hbm, bw_ref, avg_hbm, bl_hbm, bw_hbm, sum_hbm,
    tok, tgt, w, m, g, half, narrow, avg, bl, bw, tsend, trecv, lsem, osem, *sum_refs,
):
    rep, shard = lax.axis_index("rep"), lax.axis_index("shard")
    x, zl, y = rep // 8, rem(rep // 4, 2), rem(rep, 4)
    zh, core = shard // 2, rem(shard, 2)
    right = (rep, 2 * rem(zh + 1, 4) + core)
    left = (rep, 2 * rem(zh + 3, 4) + core)
    partner = (rep, 2 * zh + 1 - core)
    pair_id = (8 * x + 4 * (1 - zl) + y, shard)

    def along_x(d):
        return (8 * rem(x + d, 4) + 4 * zl + y, shard)

    def along_y(d):
        return (8 * x + 4 * zl + rem(y + d, 4), shard)

    place = (((x, along_x), (y, along_y)), pair_id)
    per = len(Sum.sizes) + 2
    first = Sum(sum_refs[:per], place, 2, F32)
    second = Sum(sum_refs[per : 2 * per], place, 2, BF16)
    even = Sum(sum_refs[2 * per : 3 * per], place, 1, BF16)
    odd = Sum(sum_refs[3 * per :], place, 1, BF16)

    def into(total):
        def store(q, g, block):
            total.own[GROUPS * q + g] = block

        return store

    def into_half(total):
        def store(q, g, block):
            total.own[GROUPS // 2 * q + g // 2] = block

        return store


    loads = [
        pltpu.make_async_copy(tok_hbm.at[0], tok.at[0, 0, core], lsem.at[0]),
        pltpu.make_async_copy(w_hbm, w, lsem.at[1]),
        pltpu.make_async_copy(m_hbm, m, lsem.at[2]),
        pltpu.make_async_copy(tgt_hbm, tgt, lsem.at[3]),
        pltpu.make_async_copy(tok_hbm.at[1], tok.at[1, 0, core], lsem.at[4]),
    ]
    for load in loads:
        load.start()

    peers = [right, left, partner, pair_id] + [f(d) for f in (along_x, along_y) for d in (1, 2, 3)]
    barrier = pltpu.get_barrier_semaphore()
    for peer in peers:
        pl.semaphore_signal(barrier, inc=1, device_id=peer, device_id_type=MESH)
    pl.semaphore_wait(barrier, len(peers))

    def move(step, relay, src, dst, recv, device):
        pltpu.make_async_remote_copy(
            src_ref=src,
            dst_ref=dst,
            send_sem=tsend.at[step, relay],
            recv_sem=recv,
            device_id=device,
            device_id_type=MESH,
        ).start()

    def drain(step, relay):
        everything = tok.at[step, 0, 0] if relay else tok.at[step, pl.ds(0, 3)]
        pltpu.make_async_remote_copy(
            src_ref=everything,
            dst_ref=everything,
            send_sem=tsend.at[step, relay],
            recv_sem=trecv.at[step, 0, 0, 0],
            device_id=partner,
            device_id_type=MESH,
        ).wait_send()

    def came(recv, dst):
        pltpu.make_async_remote_copy(
            src_ref=dst,
            dst_ref=dst,
            send_sem=tsend.at[0, 0],
            recv_sem=recv,
            device_id=partner,
            device_id_type=MESH,
        ).wait_recv()

    def send_own(step, turn):
        lower, upper = tok.at[step, 0, core, 0], tok.at[step, 0, core, 1]
        turns = (((lower, 1, 0, right), (upper, 2, 1, left)), ((upper, 1, 1, right), (lower, 2, 0, left)))
        for src, chip, part, device in turns[turn]:
            move(step, 0, src, tok.at[step, chip, core, part], trecv.at[step, chip, core, part], device)
        if turn == 0:
            both = tok.at[step, 0, core]
            move(step, 0, both, both, trecv.at[step, 0, core, 0], partner)

    waves = {1: ((1, 0), (2, 1)), 2: ((1, 1), (2, 0)), 3: ((3, 0), (3, 1))}

    def receive(step, wave):
        for k, (chip, part) in enumerate(waves[wave]):
            here, recv = tok.at[step, chip, core, part], trecv.at[step, chip, core, part]
            came(recv, here)
            if wave == 1:
                move(step, 1, here, tok.at[step, 3, core, part], trecv.at[step, 3, core, part], (right, left)[k])
            move(step, 0, here, here, recv, partner)

    def receive_partner(step, wave):
        if wave == 0:
            came(trecv.at[step, 0, 1 - core, 0], tok.at[step, 0, 1 - core])
            return
        for chip, part in waves[wave]:
            came(trecv.at[step, chip, 1 - core, part], tok.at[step, chip, 1 - core, part])

    scaling = 1.0 / math.sqrt(D)
    root = math.sqrt(2.0 / math.pi)

    def compute(step, chip):
        block = jnp.concatenate([tok[step, chip, c].reshape(D, TOKS) for c in range(2)], axis=1)
        value = jnp.dot(half[...], block, preferred_element_type=F32) * scaling
        start = rem(zh + (0, 3, 1, 2)[chip], 4) * (2 * TOKS)
        wanted = tgt[step, :, pl.ds(pl.multiple_of(start, 2 * TOKS), 2 * TOKS)].astype(F32)
        square = value * value
        curve = jnp.tanh(root * value * (1.0 + 0.044715 * square))
        gate = 0.5 * (1.0 + curve)
        slope = gate + 0.5 * value * (1.0 - curve * curve) * (root * (1.0 + 3 * 0.044715 * square))
        grad = ((value * gate - wanted) * slope * scaling).astype(BF16)
        part = lax.dot_general(grad, block, (((1,), (1,)), ((), ())), preferred_element_type=F32)
        if chip == 0:
            g[...] = part
        else:
            g[...] += part

    share = 1.0 / REPS
    every, ends = range(GROUPS), range(4)
    loads[0].wait()
    send_own(0, 0)
    loads[1].wait()
    half[...] = w[...].astype(BF16)
    pack(w, narrow, into(first), every, ends)
    first.s1()
    loads[2].wait()
    loads[3].wait()
    loads[4].wait()

    receive_partner(0, 0)
    send_own(0, 1)
    first.s1b()
    compute(0, 0)
    first.s2()
    first.s3()

    receive(0, 1)
    first.s4()
    receive(0, 2)
    receive_partner(0, 1)
    receive_partner(0, 2)
    compute(0, 1)
    compute(0, 2)
    drain(0, 1)
    send_own(1, 0)
    first.s5()

    receive(0, 3)
    receive_partner(0, 3)
    compute(0, 3)
    send_own(1, 1)
    m[...] = momentum_decay * m[...] + g[...]
    half[...] = (w[...] - learn_rate * m[...]).astype(BF16)
    pack(m, narrow, into(second), every, ends)
    second.s1()

    receive_partner(1, 0)
    compute(1, 0)
    second.s1b()
    second.s2()

    receive(1, 1)
    second.s3()
    first.s6()
    first.s6b()
    second.s4()
    receive(1, 2)
    first.s7()
    receive_partner(1, 1)
    receive_partner(1, 2)
    compute(1, 1)
    compute(1, 2)

    receive(1, 3)
    second.s5()
    receive_partner(1, 3)
    compute(1, 3)
    pack(g, narrow, into_half(even), every[::2], ends[::2])
    even.s1()
    pack(g, narrow, into_half(odd), every[1::2], ends[1::2])
    odd.s1()
    m[...] = momentum_decay * m[...] + g[...]
    even.flush()
    odd.flush()
    even.s1b()
    odd.s1b()
    even.s2()
    odd.s2()
    even.s3()
    odd.s3()
    second.s6()
    second.s6b()
    even.s4()
    odd.s4()
    even.s5()
    odd.s5()
    second.s7()
    even.s6()
    odd.s6()
    first.s8()
    second.s8()

    same = lax.broadcasted_iota(jnp.int32, (COLS, COLS), 0) == lax.broadcasted_iota(jnp.int32, (COLS, COLS), 1)
    column = jnp.sum(jnp.where(same, bw_ref[...], 0.0), axis=1, keepdims=True)
    bw[...] = jnp.broadcast_to(column, (COLS, LANES))

    def sums(block):
        w0 = first.full[block].astype(F32)
        m1 = second.full[block].astype(F32)
        average = w0 - (learn_rate * (1.0 + momentum_decay)) * m1
        return average * share, m1 * (momentum_decay * share)

    def base(q, carry):
        rows = pl.ds(pl.multiple_of(q * SUB, SUB), SUB)
        part = bw[rows, :]
        for k in range(GROUPS):
            columns = slice(LANES * k, LANES * (k + 1))
            average, mean = sums(GROUPS * q + k)
            avg[rows, columns] = average
            bl[rows, columns] = part * mean + (1.0 - part) * m[rows, columns]
        return carry

    lax.fori_loop(0, 5, base, 0)
    for b in range(2):
        rows = slice(TAILROWS * b, TAILROWS * (b + 1))
        average, mean = (tail(lambda block: sums(block)[k]) for k in range(2))
        if b:
            average, mean = pltpu.roll(average, TAIL, 1), pltpu.roll(mean, TAIL, 1)
        part = bw[rows, :TAIL]
        avg[rows, LAST] = average[:, :TAIL]
        bl[rows, LAST] = part * mean[:, :TAIL] + (1.0 - part) * m[rows, LAST]
    outs = [
        pltpu.make_async_copy(avg, avg_hbm, lsem.at[0]),
        pltpu.make_async_copy(bl, bl_hbm, lsem.at[1]),
        pltpu.make_async_copy(bw, bw_hbm, lsem.at[2]),
    ]
    for out in outs:
        out.start()

    even.s6b()
    odd.s6b()
    even.s7()
    odd.s7()
    even.s8()

    def store(k, total):
        for part in range(4):
            here = pl.ds(8 * part, 8)
            outs.append(pltpu.make_async_copy(total.full.at[here], sum_hbm.at[k, here], osem.at[k, part]))
            outs[-1].start()

    store(0, even)
    odd.s8()
    store(1, odd)
    def end_sends():
        drain(0, 0)
        drain(1, 0)
        drain(1, 1)
        for total in (first, second, even, odd):
            total.flush()

    def end_outs():
        for out in outs:
            out.wait()

    end_sends()
    end_outs()


def finish(avg_hbm, bl_hbm, bw_hbm, sum_hbm, avg_out, bl_out, avg, bl, bw, total, sem):
    rows = [pl.ds(SUB * q, SUB) for q in range(5)]
    small = [
        pltpu.make_async_copy(sum_hbm.at[:, pl.ds(30, 2)], total.at[:, pl.ds(30, 2)], sem.at[0]),
        pltpu.make_async_copy(bw_hbm, bw, sem.at[1]),
    ]
    loads = [
        [
            pltpu.make_async_copy(sum_hbm.at[:, pl.ds(6 * q, 6)], total.at[:, pl.ds(6 * q, 6)], sem.at[2 + q]),
            pltpu.make_async_copy(avg_hbm.at[rows[q]], avg.at[rows[q]], sem.at[7 + q]),
            pltpu.make_async_copy(bl_hbm.at[rows[q]], bl.at[rows[q]], sem.at[12 + q]),
        ]
        for q in range(5)
    ]
    for copy in small + sum(loads, []):
        copy.start()
    share = 1.0 / REPS
    for copy in small:
        copy.wait()
    ends = [tail(lambda block: total[block % 2, block // 2].astype(F32)) * share]
    ends.append(pltpu.roll(ends[0], TAIL, 1))
    outs = []
    for q in range(5):
        for copy in loads[q]:
            copy.wait()
        part = bw[rows[q], :] * share
        for k in range(GROUPS):
            columns = slice(LANES * k, LANES * (k + 1))
            value = total[k % 2, 6 * q + k // 2].astype(F32)
            avg[rows[q], columns] = avg[rows[q], columns] - (learn_rate * share) * value
            bl[rows[q], columns] = bl[rows[q], columns] + part * value
        for b in range(2):
            start, stop = max(SUB * q, TAILROWS * b), min(SUB * (q + 1), TAILROWS * (b + 1))
            if start < stop:
                here = slice(start, stop)
                value = ends[b][start - TAILROWS * b : stop - TAILROWS * b, :TAIL]
                avg[here, LAST] = avg[here, LAST] - learn_rate * value
                bl[here, LAST] = bl[here, LAST] + bw[here, :TAIL] * value
        for source, out, slot in ((avg, avg_out, 17 + q), (bl, bl_out, 22 + q)):
            outs.append(pltpu.make_async_copy(source.at[rows[q]], out.at[rows[q]], sem.at[slot]))
            outs[-1].start()
    for out in outs:
        out.wait()


def local(params, momentum, tokens, targets, blend_weight):
    anywhere = pl.BlockSpec(memory_space=pl.ANY)
    whole = jax.ShapeDtypeStruct((COLS, D), F32)
    parts = pl.pallas_call(
        kernel,
        out_shape=[
            whole,
            whole,
            jax.ShapeDtypeStruct((COLS, LANES), F32),
            jax.ShapeDtypeStruct((2, 32, SUB, LANES), BF16),
        ],
        in_specs=[anywhere] * 4 + [pl.BlockSpec(memory_space=pltpu.VMEM)],
        out_specs=[anywhere] * 4,
        scratch_shapes=[
            pltpu.VMEM((2, 4, 2, 2, D // 2, TOKS), BF16),
            pltpu.VMEM((2, COLS, 1024), BF16),
            pltpu.VMEM((COLS, D), F32),
            pltpu.VMEM((COLS, D), F32),
            pltpu.VMEM((COLS, D), F32),
            pltpu.VMEM((COLS, D), BF16),
            pltpu.VMEM((COLS, LANES), F32),
            pltpu.VMEM((COLS, D), F32),
            pltpu.VMEM((COLS, D), F32),
            pltpu.VMEM((COLS, LANES), F32),
            pltpu.SemaphoreType.DMA((2, 2)),
            pltpu.SemaphoreType.DMA((2, 4, 2, 2)),
            pltpu.SemaphoreType.DMA((5,)),
            pltpu.SemaphoreType.DMA((2, 4)),
            *Sum.scratch(2, F32),
            *Sum.scratch(2, BF16),
            *Sum.scratch(1, BF16),
            *Sum.scratch(1, BF16),
        ],
        compiler_params=pltpu.CompilerParams(
            collective_id=0, has_side_effects=True, vmem_limit_bytes=67043328
        ),
        name="window",
    )(
        params[0].T,
        momentum[0].T,
        tokens[0].transpose(0, 2, 1).reshape(2, 2, D // 2, TOKS),
        targets[0].transpose(0, 2, 1),
        blend_weight.reshape(1, COLS),
    )
    averaged, blended = pl.pallas_call(
        finish,
        out_shape=[whole, whole],
        in_specs=[anywhere] * 4,
        out_specs=[anywhere] * 2,
        scratch_shapes=[
            pltpu.VMEM((COLS, D), F32),
            pltpu.VMEM((COLS, D), F32),
            pltpu.VMEM((COLS, LANES), F32),
            pltpu.VMEM((2, 32, SUB, LANES), BF16),
            pltpu.SemaphoreType.DMA((27,)),
        ],
        name="finish",
    )(*parts)
    return averaged.T, blended.T[None]


def solution(mesh):
    return jax.shard_map(
        local,
        mesh=mesh,
        in_specs=(
            P("rep", None, "shard"),
            P("rep", None, "shard"),
            P("rep", None, "shard", None),
            P("rep", None, None, "shard"),
            P("shard"),
        ),
        out_specs=(P(None, "shard"), P("rep", None, "shard")),
        check_vma=False,
    )
```
